128 devices in a mesh: grp: 16 (over z, y), mem: 8 (over x, core).
Axes of the slice: x: 4, y: 4, z: 4, core: 2. Of those that a mesh axis runs over, the one named last changes fastest.
Arguments:
- queries: bfloat16 [32768, 2048], P(('grp', 'mem')), may hold values from -6 to 6
- keys: bfloat16 [32768, 2048], P(('grp', 'mem')), may hold values from -6 to 6
- values: bfloat16 [32768, 2048], P(('grp', 'mem')), may hold values from -6 to 6
- grad_out: bfloat16 [32768, 2048], P(('grp', 'mem')), may hold values from -0.0625 to 0.0625
- log_decay: float32 [8, 32768], P(None, ('grp', 'mem')), may hold values from -1.6 to 0
Outputs:
- grad_queries: bfloat16 [32768, 2048], P(('grp', 'mem'))
- grad_keys: bfloat16 [32768, 2048], P(('grp', 'mem'))
- grad_values: bfloat16 [32768, 2048], P(('grp', 'mem'))
The draws below stay inside these ranges and needn't reach their ends.
All inputs are finite; a program needn't handle non-finite values.
Results may differ from the reference program's by a relative error of at most 0.0052.
Values sent between devices are 32-bit elements; how exact they have to be, the bound alone decides.
A program may use at most 128 MiB of HBM per device.

```python
import jax
import jax.numpy as jnp
from jax import lax

HEAD_COUNT = 8
DK = 256
DV = 256
BLOCK = 128
TOK_DEV = 256
SEQUENCE_TOKENS = 32768


def draw_log_decay(key, part):
    base_key = jax.random.fold_in(key, 7)
    key_collection = jax.random.split(base_key, 6)
    order = jax.random.permutation(key_collection[0], HEAD_COUNT)
    fast_count = HEAD_COUNT // 2
    fast = order < fast_count
    fast_rate = jnp.exp(jax.random.uniform(key_collection[1], (HEAD_COUNT,), jnp.float32, jnp.log(1.0 / 50.0), jnp.log(1.0 / 30.0)))
    slow_rate = 0.3 / SEQUENCE_TOKENS
    decay_rates = jnp.where(fast, fast_rate, slow_rate)
    approximate = jnp.exp(jax.random.uniform(key_collection[2], (HEAD_COUNT, SEQUENCE_TOKENS), jnp.float32, jnp.log(0.5), jnp.log(2.0)))
    device_count = SEQUENCE_TOKENS // TOK_DEV
    device_factor = jnp.exp(jax.random.uniform(key_collection[3], (HEAD_COUNT, device_count), jnp.float32, jnp.log(0.5), jnp.log(2.0)))
    device_complete = jnp.repeat(device_factor, TOK_DEV, axis=1)
    spike_start = jax.random.randint(key_collection[4], (HEAD_COUNT, 2), 0, SEQUENCE_TOKENS)
    spike_length = jax.random.uniform(key_collection[5], (HEAD_COUNT, 2), jnp.float32, 0.22, 0.69)
    token_positions = jnp.arange(SEQUENCE_TOKENS)
    match_count = (token_positions[None, None, :] == spike_start[:, :, None]).astype(jnp.float32)
    spike_run = jnp.sum(match_count * spike_length[:, :, None], axis=1)
    return (-(decay_rates[:, None] * approximate * device_complete) - spike_run).astype(jnp.float32)


def block_levels(key, shape, cuts, least, high):
    level = 1.0
    for axis_at, parts in cuts:
        steps = jax.random.uniform(jax.random.fold_in(jax.random.fold_in(key, 6), axis_at), (parts,), jnp.float32, least / len(cuts), high / len(cuts))
        level = level * jnp.repeat(jnp.exp(steps), shape[axis_at] // parts).reshape((-1,) + (1,) * (len(shape) - 1 - axis_at))
    return level


def gaussian(stream_key, extent, scale, limit, pieces=(), kind=jnp.bfloat16):
    gain = block_levels(stream_key, extent, pieces, -0.22, 0.18) if pieces else 1.0
    values = jax.random.normal(stream_key, extent, jnp.float32) * scale * gain
    return jnp.minimum(jnp.maximum(values, -limit), limit).astype(kind)


def setup_inputs(seed: int = 0) -> dict:
    splits = jax.random.split(jax.random.key(seed), 6)
    queries = gaussian(splits[0], (SEQUENCE_TOKENS, HEAD_COUNT * DK), 1.0, 6.0, ((0, 128),))
    keys = gaussian(splits[1], (SEQUENCE_TOKENS, HEAD_COUNT * DK), 1.0, 6.0, ((0, 128),))
    values = gaussian(splits[2], (SEQUENCE_TOKENS, HEAD_COUNT * DV), 1.0, 6.0, ((0, 128),))
    grad_out = gaussian(splits[3], (SEQUENCE_TOKENS, HEAD_COUNT * DV), (2 * SEQUENCE_TOKENS ** -0.5), 0.0625, ((0, 128),))
    log_decay = draw_log_decay(jax.random.fold_in(splits[5], 71), 0)
    return dict(queries=queries, keys=keys, values=values, grad_out=grad_out, log_decay=log_decay)


def block_factors(logs):
    cumul = jnp.cumsum(logs, axis=-1)
    ends = cumul[:, -1]
    width = logs.shape[-1]
    lower = jnp.tril(jnp.ones((width, width), dtype=bool))
    spread = cumul[:, :, None] - cumul[:, None, :]
    decay = jnp.where(lower, jnp.exp(jnp.where(lower, spread, 0.0)), 0.0)
    return cumul, ends, decay


def reference(queries, keys, values, grad_out, log_decay):
    count = SEQUENCE_TOKENS // BLOCK
    scale = DK ** -0.5
    query_blocks = queries.reshape(count, BLOCK, HEAD_COUNT, DK)
    key_blocks = keys.reshape(count, BLOCK, HEAD_COUNT, DK)
    value_blocks = values.reshape(count, BLOCK, HEAD_COUNT, DV)
    grad_blocks = grad_out.reshape(count, BLOCK, HEAD_COUNT, DV)
    log_blocks = jnp.transpose(log_decay.reshape(HEAD_COUNT, count, BLOCK), (1, 0, 2))

    def forward_step(state, inputs):
        query_now, key_now, value_now, grad_now, logs = inputs
        query32 = query_now.astype(jnp.float32)
        key32 = key_now.astype(jnp.float32)
        value32 = value_now.astype(jnp.float32)
        grad32 = grad_now.astype(jnp.float32)
        cumul, ends, decay = block_factors(logs)
        scores = jnp.einsum('the,she->hts', grad32, value32)
        weight_grad = lax.optimization_barrier((scores * decay).astype(jnp.bfloat16))
        inner = jnp.einsum('hts,shd->thd', weight_grad.astype(jnp.float32), key32)
        state_low = lax.optimization_barrier(state.astype(jnp.bfloat16))
        outer = jnp.einsum('the,hde->thd', grad32, state_low.astype(jnp.float32))
        outer = outer * jnp.exp(cumul).T[:, :, None]
        result = (scale * (inner + outer)).astype(jnp.bfloat16)
        tail = jnp.exp(ends[:, None] - cumul).T[:, :, None]
        keys_decayed = lax.optimization_barrier((key32 * tail).astype(jnp.bfloat16))
        update = jnp.einsum('shd,she->hde', keys_decayed.astype(jnp.float32), value32)
        state_next = jnp.exp(ends)[:, None, None] * state + update
        return state_next, result

    def reverse_step(state, inputs):
        query_now, key_now, value_now, grad_now, logs = inputs
        query32 = query_now.astype(jnp.float32)
        key32 = key_now.astype(jnp.float32)
        value32 = value_now.astype(jnp.float32)
        grad32 = grad_now.astype(jnp.float32)
        cumul, ends, decay = block_factors(logs)
        scores = jnp.einsum('the,she->hts', grad32, value32)
        weight_grad = lax.optimization_barrier((scores * decay).astype(jnp.bfloat16))
        attend = jnp.einsum('thd,shd->hts', query32, key32)
        weight_value = lax.optimization_barrier((attend * decay).astype(jnp.bfloat16))
        state_low = lax.optimization_barrier(state.astype(jnp.bfloat16)).astype(jnp.float32)
        tail = jnp.exp(ends[:, None] - cumul).T[:, :, None]
        key_grad = jnp.einsum('hts,thd->shd', weight_grad.astype(jnp.float32), query32)
        key_grad = key_grad + tail * jnp.einsum('she,hde->shd', value32, state_low)
        value_grad = jnp.einsum('hts,the->she', weight_value.astype(jnp.float32), grad32)
        value_grad = value_grad + tail * jnp.einsum('shd,hde->she', key32, state_low)
        queries_decayed = lax.optimization_barrier((query32 * jnp.exp(cumul).T[:, :, None]).astype(jnp.bfloat16))
        update = jnp.einsum('thd,the->hde', queries_decayed.astype(jnp.float32), grad32)
        state_next = jnp.exp(ends)[:, None, None] * state + update
        return state_next, ((scale * key_grad).astype(jnp.bfloat16), (scale * value_grad).astype(jnp.bfloat16))

    inputs = (query_blocks, key_blocks, value_blocks, grad_blocks, log_blocks)
    empty = jnp.zeros((HEAD_COUNT, DK, DV), jnp.float32)
    unused, grad_q = lax.scan(forward_step, empty, inputs)
    unused_too, pair = lax.scan(reverse_step, empty, inputs, reverse=True)
    grad_k, grad_v = pair
    return (grad_q.reshape(SEQUENCE_TOKENS, HEAD_COUNT * DK), grad_k.reshape(SEQUENCE_TOKENS, HEAD_COUNT * DK), grad_v.reshape(SEQUENCE_TOKENS, HEAD_COUNT * DV))
```

```python
import functools

import jax
import jax.numpy as jnp
from jax import lax
from jax.experimental import pallas as pl
from jax.experimental.pallas import tpu as pltpu
from jax.sharding import Mesh
from jax.sharding import PartitionSpec as P

H = 8
DK = 256
DV = 256
BLOCK = 128
AXES = ("z", "y", "x", "c")
MESH = pl.DeviceIdType.MESH
F32 = jnp.float32
BF16 = jnp.bfloat16
SHARE = 32


def two(a):
    return jnp.concatenate([a, a], axis=1)


def dot(a, b, ca, cb):
    return lax.dot_general(a, b, (((ca,), (cb,)), ((), ())), preferred_element_type=F32)


def kernel(q, k, v, g, ld, dq, dk, dv, col, en, inner, u0s, v1s, tc, pt, ct, xu, yb, pln, zb,
           sd, xd, sp, fs, dc, dx, dy, dz, wc, wx, wy, wz, s_small, r_small, s_t, r_t, s_xu, r_xu,
           s_y, r_y, s_z, r_z, s_xd, r_xd, s_f, r_f):
    iz, iy, ix, ic = (lax.axis_index(a) for a in AXES)
    other = 1 - ic

    def peer(axis, i):
        if axis == "c":
            return {"c": other}
        return {axis: lax.rem(lax.axis_index(axis) + i, 4)}

    barrier = pltpu.get_barrier_semaphore()
    pl.semaphore_signal(barrier, inc=1, device_id=peer("c", 1), device_id_type=MESH)
    for axis in ("x", "y", "z"):
        for i in (1, 2, 3):
            pl.semaphore_signal(barrier, inc=1, device_id=peer(axis, i), device_id_type=MESH)

    def remote(src, dst, ssem, rsem, axis, i):
        return pltpu.make_async_remote_copy(
            src_ref=src, dst_ref=dst, send_sem=ssem, recv_sem=rsem,
            device_id=peer(axis, i), device_id_type=MESH)

    def c_small():
        return remote(dc.at[ic], dc.at[ic], s_small.at[0], r_small.at[0], "c", 1)

    def small(buf, mine, base, axis, i):
        return remote(buf.at[mine], buf.at[mine], s_small.at[base + i], r_small.at[base + i], axis, i)

    def t_copy(h):
        rows = pl.ds(pl.multiple_of(128 * other, 128), 128)
        return remote(tc.at[h, :, rows], pt.at[h], s_t.at[h], r_t.at[h], "c", 1)

    def xu_copy(h, i):
        return remote(ct.at[h, lax.rem(ix + i, 4)], xu.at[h, ix], s_xu.at[h, i - 1], r_xu.at[h, i - 1], "x", i)

    def y_copy(h, i):
        return remote(yb.at[h, iy], yb.at[h, iy], s_y.at[h, i - 1], r_y.at[h, i - 1], "y", i)

    def z_copy(h, i):
        part = lax.div(iz + i, 4)
        return remote(pln.at[h, part], zb.at[h, iz], s_z.at[h, i - 1], r_z.at[h, i - 1], "z", i)

    def xd_copy(h, i):
        return remote(sd.at[h, lax.rem(ix + i, 4)], xd.at[h, ix], s_xd.at[h, i - 1], r_xd.at[h, i - 1], "x", i)

    def f_copy(h):
        rows = pl.ds(pl.multiple_of(128 * ic, 128), 128)
        return remote(sp.at[h], fs.at[h, :, rows], s_f.at[h], r_f.at[h], "c", 1)

    ii = lax.broadcasted_iota(jnp.int32, (BLOCK, BLOCK), 0)
    jj = lax.broadcasted_iota(jnp.int32, (BLOCK, BLOCK), 1)
    upper = jnp.where(ii <= jj, 1.0, 0.0).astype(F32)
    for b in range(2):
        cum = lax.dot_general(ld[:, b * BLOCK:(b + 1) * BLOCK], upper, (((1,), (0,)), ((), ())),
                              precision=lax.Precision.HIGHEST, preferred_element_type=F32)
        for h in range(H):
            col[h, b] = jnp.broadcast_to(cum[h:h + 1, :], (BLOCK, BLOCK)).T
        en[b] = jnp.broadcast_to(cum[:, BLOCK - 1:BLOCK], (H, DV))
    dc[ic] = en[0] + en[1]

    pl.semaphore_wait(barrier, 10)
    c_small().start()

    def products(h):
        cols = pl.ds(pl.multiple_of(h * DK, DK), DK)
        parts = []
        for b in range(2):
            rows = slice(b * BLOCK, (b + 1) * BLOCK)
            cb = col[h, b]
            hf = two(jnp.exp(cb))
            tf = two(jnp.exp(cb[BLOCK - 1:BLOCK, :] - cb))
            kd = (k[rows, cols].astype(F32) * tf).astype(BF16)
            qd = (q[rows, cols].astype(F32) * hf).astype(BF16)
            parts.append((dot(kd, v[rows, cols], 0, 0), dot(qd, g[rows, cols], 0, 0)))
        e0 = jnp.exp(en[0, pl.ds(h, 1), :])
        e1 = jnp.exp(en[1, pl.ds(h, 1), :])
        u0s[h] = parts[0][0]
        v1s[h] = parts[1][1]
        tc[h, 0] = e1 * parts[0][0] + parts[1][0]
        tc[h, 1] = e0 * parts[1][1] + parts[0][1]
        t_copy(h).start()

    def chip_total(h):
        t_copy(h).wait_recv()
        for s in range(4):
            for d in range(2):
                mine = pl.ds(pl.multiple_of(128 * ic + SHARE * s, SHARE), SHARE)
                ct[h, s, d] = (wc[2 * d, pl.ds(h, 1), :] * tc[h, d, mine, :]
                               + wc[2 * d + 1, pl.ds(h, 1), :] * pt[h, d, pl.ds(SHARE * s, SHARE), :])
        xu[h, ix] = ct[h, ix]
        for i in (1, 2, 3):
            xu_copy(h, i).start()

    def chain_total(buf, w, h):
        f = buf[h, 0, 0]
        for j in (1, 2, 3):
            f = w[j, pl.ds(h, 1), :] * f + buf[h, j, 0]
        r = buf[h, 3, 1]
        for j in (2, 1, 0):
            r = w[j, pl.ds(h, 1), :] * r + buf[h, j, 1]
        return f, r

    def row_total(h):
        for i in (1, 2, 3):
            xu_copy(h, i).wait_recv()
        f, r = chain_total(xu, wx, h)
        yb[h, iy, 0] = f
        yb[h, iy, 1] = r
        for i in (1, 2, 3):
            y_copy(h, i).start()

    def plane_total(h):
        for i in (1, 2, 3):
            y_copy(h, i).wait_recv()
        f, r = chain_total(yb, wy, h)
        pln[h, 0] = f
        pln[h, 1] = r
        zb[h, iz] = jnp.zeros((SHARE, DV), F32)
        for i in (1, 2, 3):
            z_copy(h, i).start()

    def incoming(h):
        for i in (1, 2, 3):
            z_copy(h, i).wait_recv()
        f = jnp.zeros((SHARE, DV), F32)
        r = jnp.zeros((SHARE, DV), F32)
        for j in range(4):
            zj = zb[h, j]
            f = f + wz[j, pl.ds(h, 1), :] * zj
            r = r + wz[4 + j, pl.ds(h, 1), :] * zj
        for j in range(4):
            f = f + wz[8 + j, pl.ds(h, 1), :] * yb[h, j, 0]
            r = r + wz[12 + j, pl.ds(h, 1), :] * yb[h, j, 1]
        for j in range(4):
            sd[h, j, 0] = f
            if j < 3:
                f = wx[j, pl.ds(h, 1), :] * f + xu[h, j, 0]
        for j in (3, 2, 1, 0):
            sd[h, j, 1] = r
            if j > 0:
                r = wx[j, pl.ds(h, 1), :] * r + xu[h, j, 1]
        xd[h, ix] = sd[h, ix]
        for i in (1, 2, 3):
            xd_copy(h, i).start()

    def core_state(h):
        for i in (1, 2, 3):
            xd_copy(h, i).wait_recv()
        for s in range(4):
            for d in range(2):
                mine = pl.ds(pl.multiple_of(128 * ic + SHARE * s, SHARE), SHARE)
                st = xd[h, s, d]
                fs[h, d, mine, :] = (wc[4 + 2 * d, pl.ds(h, 1), :] * st
                                     + wc[5 + 2 * d, pl.ds(h, 1), :] * pt[h, d, pl.ds(SHARE * s, SHARE), :])
                sp[h, d, pl.ds(SHARE * s, SHARE), :] = (wc[8 + 2 * d, pl.ds(h, 1), :] * st
                                                        + wc[9 + 2 * d, pl.ds(h, 1), :] * tc[h, d, mine, :])
        f_copy(h).start()

    def inside(h):
        cols = pl.ds(pl.multiple_of(h * DK, DK), DK)
        for b in range(2):
            rows = slice(b * BLOCK, (b + 1) * BLOCK)
            cb = col[h, b]
            spread = cb - cb.T
            decay = jnp.where(jj <= ii, jnp.exp(jnp.where(jj <= ii, spread, 0.0)), 0.0)
            qb, kb, vb, gb = q[rows, cols], k[rows, cols], v[rows, cols], g[rows, cols]
            wg = (dot(gb, vb, 1, 1) * decay).astype(BF16)
            wv = (dot(qb, kb, 1, 1) * decay).astype(BF16)
            inner[h, 0, rows, :] = dot(wg, kb, 1, 0)
            inner[h, 1, rows, :] = dot(wg, qb, 0, 0)
            inner[h, 2, rows, :] = dot(wv, gb, 0, 0)

    def outputs(h):
        f_copy(h).wait_recv()
        cols = pl.ds(pl.multiple_of(h * DK, DK), DK)
        e0 = jnp.exp(en[0, pl.ds(h, 1), :])
        e1 = jnp.exp(en[1, pl.ds(h, 1), :])
        sf = fs[h, 0]
        sr = fs[h, 1]
        states = (sf.astype(BF16), (e0 * sf + u0s[h]).astype(BF16))
        grads = ((e1 * sr + v1s[h]).astype(BF16), sr.astype(BF16))
        scale = DK ** -0.5
        for b in range(2):
            rows = slice(b * BLOCK, (b + 1) * BLOCK)
            cb = col[h, b]
            hf = two(jnp.exp(cb))
            tf = two(jnp.exp(cb[BLOCK - 1:BLOCK, :] - cb))
            oq = dot(g[rows, cols], states[b], 1, 1)
            ok = dot(v[rows, cols], grads[b], 1, 1)
            ov = dot(k[rows, cols], grads[b], 1, 0)
            dq[rows, cols] = (scale * (inner[h, 0, rows, :] + hf * oq)).astype(BF16)
            dk[rows, cols] = (scale * (inner[h, 1, rows, :] + tf * ok)).astype(BF16)
            dv[rows, cols] = (scale * (inner[h, 2, rows, :] + tf * ov)).astype(BF16)

    def core_weights():
        c_small().wait_recv()
        me = dc[ic]
        ot = dc[other]
        first = ic == 0
        one = jnp.ones((H, DV), F32)
        zero = jnp.zeros((H, DV), F32)
        eme = jnp.exp(me)
        eot = jnp.exp(ot)
        wc[0] = jnp.where(first, eot, one)
        wc[1] = jnp.where(first, one, eme)
        wc[2] = jnp.where(first, one, eot)
        wc[3] = jnp.where(first, eme, one)
        wc[4] = jnp.where(first, one, eot)
        wc[5] = jnp.where(first, zero, one)
        wc[6] = jnp.where(first, eot, one)
        wc[7] = jnp.where(first, one, zero)
        wc[8] = jnp.where(first, eme, one)
        wc[9] = jnp.where(first, one, zero)
        wc[10] = jnp.where(first, one, eme)
        wc[11] = jnp.where(first, zero, one)
        dx[ix] = me + ot
        for i in (1, 2, 3):
            small(dx, ix, 0, "x", i).start()

    def row_weights():
        for i in (1, 2, 3):
            small(dx, ix, 0, "x", i).wait_recv()
        for j in range(4):
            wx[j] = jnp.exp(dx[j])
        dy[iy] = (dx[0] + dx[1]) + (dx[2] + dx[3])
        for i in (1, 2, 3):
            small(dy, iy, 3, "y", i).start()

    def plane_weights():
        for i in (1, 2, 3):
            small(dy, iy, 3, "y", i).wait_recv()
        for j in range(4):
            wy[j] = jnp.exp(dy[j])
        dz[iz] = (dy[0] + dy[1]) + (dy[2] + dy[3])
        for i in (1, 2, 3):
            small(dz, iz, 6, "z", i).start()

    def prefix_weights():
        for i in (1, 2, 3):
            small(dz, iz, 6, "z", i).wait_recv()
        zero = jnp.zeros((H, DV), F32)
        before = zero
        after = zero
        for j in range(4):
            before = before + jnp.where(j < iy, dy[j], 0.0)
            after = after + jnp.where(j > iy, dy[j], 0.0)
        for j in range(4):
            zf, zr, yf, yr = before, after, zero, zero
            for m in range(4):
                if m > j:
                    zf = zf + jnp.where(m < iz, dz[m], 0.0)
                    yf = yf + jnp.where(m < iy, dy[m], 0.0)
                if m < j:
                    zr = zr + jnp.where(m > iz, dz[m], 0.0)
                    yr = yr + jnp.where(m > iy, dy[m], 0.0)
            wz[j] = jnp.where(j < iz, jnp.exp(zf), 0.0)
            wz[4 + j] = jnp.where(j > iz, jnp.exp(zr), 0.0)
            wz[8 + j] = jnp.where(j < iy, jnp.exp(yf), 0.0)
            wz[12 + j] = jnp.where(j > iy, jnp.exp(yr), 0.0)

    def first_loop(t, carry):
        @pl.when(t < H)
        def _():
            products(t)

        @pl.when(t == 0)
        def _():
            core_weights()

        @pl.when(t == 3)
        def _():
            row_weights()

        @pl.when(t == 6)
        def _():
            plane_weights()

        @pl.when(t >= 1)
        def _():
            chip_total(t - 1)
        return carry

    lax.fori_loop(0, H + 1, first_loop, 0)
    prefix_weights()

    def second_loop(t, carry):
        @pl.when(t < H)
        def _():
            row_total(t)

        @pl.when((t >= 1) & (t < H + 1))
        def _():
            plane_total(t - 1)

        @pl.when(t >= 2)
        def _():
            incoming(t - 2)

        @pl.when(t < H)
        def _():
            inside(t)
        return carry

    lax.fori_loop(0, H + 2, second_loop, 0)

    def third_loop(t, carry):
        @pl.when(t < H)
        def _():
            core_state(t)

        @pl.when(t >= 1)
        def _():
            outputs(t - 1)
        return carry

    lax.fori_loop(0, H + 1, third_loop, 0)

    def drain(h, carry):
        t_copy(h).wait_send()
        f_copy(h).wait_send()
        for i in (1, 2, 3):
            xu_copy(h, i).wait_send()
            y_copy(h, i).wait_send()
            z_copy(h, i).wait_send()
            xd_copy(h, i).wait_send()
        return carry

    lax.fori_loop(0, H, drain, 0)
    c_small().wait_send()
    for i in (1, 2, 3):
        small(dx, ix, 0, "x", i).wait_send()
        small(dy, iy, 3, "y", i).wait_send()
        small(dz, iz, 6, "z", i).wait_send()


def body(queries, keys, values, grad_out, log_decay):
    vmem = pl.BlockSpec(memory_space=pltpu.VMEM)
    shape = jax.ShapeDtypeStruct(queries.shape, BF16)
    tile = pltpu.VMEM
    dma = pltpu.SemaphoreType.DMA
    return pl.pallas_call(
        kernel,
        out_shape=(shape, shape, shape),
        in_specs=[vmem] * 5,
        out_specs=(vmem, vmem, vmem),
        scratch_shapes=[
            tile((H, 2, BLOCK, BLOCK), F32),
            tile((2, H, DV), F32),
            tile((H, 3, 2 * BLOCK, DK), F32),
            tile((H, DK, DV), F32),
            tile((H, DK, DV), F32),
            tile((H, 2, DK, DV), F32),
            tile((H, 2, DK // 2, DV), F32),
            tile((H, 4, 2, SHARE, DV), F32),
            tile((H, 4, 2, SHARE, DV), F32),
            tile((H, 4, 2, SHARE, DV), F32),
            tile((H, 2, SHARE, DV), F32),
            tile((H, 4, SHARE, DV), F32),
            tile((H, 4, 2, SHARE, DV), F32),
            tile((H, 4, 2, SHARE, DV), F32),
            tile((H, 2, DK // 2, DV), F32),
            tile((H, 2, DK, DV), F32),
            tile((2, H, DV), F32),
            tile((4, H, DV), F32),
            tile((4, H, DV), F32),
            tile((4, H, DV), F32),
            tile((12, H, DV), F32),
            tile((4, H, DV), F32),
            tile((4, H, DV), F32),
            tile((16, H, DV), F32),
            dma((10,)), dma((10,)),
            dma((H,)), dma((H,)),
            dma((H, 3)), dma((H, 3)),
            dma((H, 3)), dma((H, 3)),
            dma((H, 3)), dma((H, 3)),
            dma((H, 3)), dma((H, 3)),
            dma((H,)), dma((H,)),
        ],
        compiler_params=pltpu.CompilerParams(
            collective_id=0, has_side_effects=True, vmem_limit_bytes=60 * 1024 * 1024),
    )(queries, keys, values, grad_out, log_decay)


def solution(mesh):
    torus = Mesh(mesh.devices.reshape(4, 4, 4, 2), AXES)
    rows = P(AXES, None)
    return jax.shard_map(
        body,
        mesh=torus,
        in_specs=(rows, rows, rows, rows, P(None, AXES)),
        out_specs=(rows, rows, rows),
        check_vma=False,
    )
```

```python
import functools

import jax
import jax.numpy as jnp
from jax import lax
from jax.experimental import pallas as pl
from jax.experimental.pallas import tpu as pltpu
from jax.sharding import Mesh
from jax.sharding import PartitionSpec as P

H = 8
DK = 256
DV = 256
BLOCK = 128
AXES = ("z", "y", "x", "c")
MESH = pl.DeviceIdType.MESH
F32 = jnp.float32
BF16 = jnp.bfloat16
SHARE = 32
EARLY = 3


def two(a):
    return jnp.concatenate([a, a], axis=1)


def dot(a, b, ca, cb):
    return lax.dot_general(a, b, (((ca,), (cb,)), ((), ())), preferred_element_type=F32)


def kernel(qh, kh, vh, gh, ld, dq, dk, dv, q, k, v, g, s_in, col, en, inner, u0s, v1s, tc, pt, ct, xu, yb, pln, zb,
           sd, xd, sp, fs, dc, dx, dy, dz, wc, wx, wy, wz, s_small, r_small, s_t, r_t, s_xu, r_xu,
           s_y, r_y, s_z, r_z, s_xd, r_xd, s_f, r_f):
    iz, iy, ix, ic = (lax.axis_index(a) for a in AXES)
    other = 1 - ic

    def peer(axis, i):
        if axis == "c":
            return {"c": other}
        return {axis: lax.rem(lax.axis_index(axis) + i, 4)}

    loads = [pltpu.make_async_copy(a, b, s_in.at[i])
             for i, (a, b) in enumerate(((kh, k), (vh, v), (qh, q), (gh, g)))]
    for load in loads:
        load.start()
    barrier = pltpu.get_barrier_semaphore()
    pl.semaphore_signal(barrier, inc=1, device_id=peer("c", 1), device_id_type=MESH)
    for axis in ("x", "y", "z"):
        for i in (1, 2, 3):
            pl.semaphore_signal(barrier, inc=1, device_id=peer(axis, i), device_id_type=MESH)

    def remote(src, dst, ssem, rsem, axis, i):
        return pltpu.make_async_remote_copy(
            src_ref=src, dst_ref=dst, send_sem=ssem, recv_sem=rsem,
            device_id=peer(axis, i), device_id_type=MESH)

    def c_small():
        return remote(dc.at[ic], dc.at[ic], s_small.at[0], r_small.at[0], "c", 1)

    def small(buf, mine, base, axis, i):
        return remote(buf.at[mine], buf.at[mine], s_small.at[base + i], r_small.at[base + i], axis, i)

    def t_copy(h):
        rows = pl.ds(pl.multiple_of(128 * other, 128), 128)
        return remote(tc.at[h, :, rows], pt.at[h], s_t.at[h], r_t.at[h], "c", 1)

    def xu_copy(h, i):
        return remote(ct.at[h, lax.rem(ix + i, 4)], xu.at[h, ix], s_xu.at[h, i - 1], r_xu.at[h, i - 1], "x", i)

    def y_copy(h, i):
        return remote(yb.at[h, iy], yb.at[h, iy], s_y.at[h, i - 1], r_y.at[h, i - 1], "y", i)

    def z_copy(h, i):
        part = lax.div(iz + i, 4)
        return remote(pln.at[h, part], zb.at[h, iz], s_z.at[h, i - 1], r_z.at[h, i - 1], "z", i)

    def xd_copy(h, i):
        return remote(sd.at[h, lax.rem(ix + i, 4)], xd.at[h, ix], s_xd.at[h, i - 1], r_xd.at[h, i - 1], "x", i)

    def f_copy(h):
        rows = pl.ds(pl.multiple_of(128 * ic, 128), 128)
        return remote(sp.at[h], fs.at[h, :, rows], s_f.at[h], r_f.at[h], "c", 1)

    ii = lax.broadcasted_iota(jnp.int32, (BLOCK, BLOCK), 0)
    jj = lax.broadcasted_iota(jnp.int32, (BLOCK, BLOCK), 1)
    upper = jnp.where(ii <= jj, 1.0, 0.0).astype(F32)
    for b in range(2):
        cum = lax.dot_general(ld[:, b * BLOCK:(b + 1) * BLOCK], upper, (((1,), (0,)), ((), ())),
                              precision=lax.Precision.HIGHEST, preferred_element_type=F32)
        for h in range(H):
            col[h, b] = jnp.broadcast_to(cum[h:h + 1, :], (BLOCK, BLOCK)).T
        en[b] = jnp.broadcast_to(cum[:, BLOCK - 1:BLOCK], (H, DV))
    dc[ic] = en[0] + en[1]
    for load in loads:
        load.wait()

    def products(h):
        cols = pl.ds(pl.multiple_of(h * DK, DK), DK)
        parts = []
        for b in range(2):
            rows = slice(b * BLOCK, (b + 1) * BLOCK)
            cb = col[h, b]
            hf = two(jnp.exp(cb))
            tf = two(jnp.exp(cb[BLOCK - 1:BLOCK, :] - cb))
            kd = (k[rows, cols].astype(F32) * tf).astype(BF16)
            qd = (q[rows, cols].astype(F32) * hf).astype(BF16)
            parts.append((dot(kd, v[rows, cols], 0, 0), dot(qd, g[rows, cols], 0, 0)))
        e0 = jnp.exp(en[0, pl.ds(h, 1), :])
        e1 = jnp.exp(en[1, pl.ds(h, 1), :])
        u0s[h] = parts[0][0]
        v1s[h] = parts[1][1]
        tc[h, 0] = e1 * parts[0][0] + parts[1][0]
        tc[h, 1] = e0 * parts[1][1] + parts[0][1]

    def chip_total(h):
        t_copy(h).wait_recv()
        for s in range(4):
            for d in range(2):
                mine = pl.ds(pl.multiple_of(128 * ic + SHARE * s, SHARE), SHARE)
                ct[h, s, d] = (wc[2 * d, pl.ds(h, 1), :] * tc[h, d, mine, :]
                               + wc[2 * d + 1, pl.ds(h, 1), :] * pt[h, d, pl.ds(SHARE * s, SHARE), :])
        xu[h, ix] = ct[h, ix]
        for i in (1, 2, 3):
            xu_copy(h, i).start()

    def chain_total(buf, w, h):
        f = buf[h, 0, 0]
        for j in (1, 2, 3):
            f = w[j, pl.ds(h, 1), :] * f + buf[h, j, 0]
        r = buf[h, 3, 1]
        for j in (2, 1, 0):
            r = w[j, pl.ds(h, 1), :] * r + buf[h, j, 1]
        return f, r

    def row_total(h):
        for i in (1, 2, 3):
            xu_copy(h, i).wait_recv()
        f, r = chain_total(xu, wx, h)
        yb[h, iy, 0] = f
        yb[h, iy, 1] = r
        for i in (1, 2, 3):
            y_copy(h, i).start()

    def plane_total(h):
        for i in (1, 2, 3):
            y_copy(h, i).wait_recv()
        f, r = chain_total(yb, wy, h)
        pln[h, 0] = f
        pln[h, 1] = r
        zb[h, iz] = jnp.zeros((SHARE, DV), F32)
        for i in (1, 2, 3):
            z_copy(h, i).start()

    def incoming(h):
        for i in (1, 2, 3):
            z_copy(h, i).wait_recv()
        f = jnp.zeros((SHARE, DV), F32)
        r = jnp.zeros((SHARE, DV), F32)
        for j in range(4):
            zj = zb[h, j]
            f = f + wz[j, pl.ds(h, 1), :] * zj
            r = r + wz[4 + j, pl.ds(h, 1), :] * zj
        for j in range(4):
            f = f + wz[8 + j, pl.ds(h, 1), :] * yb[h, j, 0]
            r = r + wz[12 + j, pl.ds(h, 1), :] * yb[h, j, 1]
        for j in range(4):
            sd[h, j, 0] = f
            if j < 3:
                f = wx[j, pl.ds(h, 1), :] * f + xu[h, j, 0]
        for j in (3, 2, 1, 0):
            sd[h, j, 1] = r
            if j > 0:
                r = wx[j, pl.ds(h, 1), :] * r + xu[h, j, 1]
        xd[h, ix] = sd[h, ix]
        for i in (1, 2, 3):
            xd_copy(h, i).start()

    def core_state(h):
        for i in (1, 2, 3):
            xd_copy(h, i).wait_recv()
        for s in range(4):
            for d in range(2):
                mine = pl.ds(pl.multiple_of(128 * ic + SHARE * s, SHARE), SHARE)
                st = xd[h, s, d]
                fs[h, d, mine, :] = (wc[4 + 2 * d, pl.ds(h, 1), :] * st
                                     + wc[5 + 2 * d, pl.ds(h, 1), :] * pt[h, d, pl.ds(SHARE * s, SHARE), :])
                sp[h, d, pl.ds(SHARE * s, SHARE), :] = (wc[8 + 2 * d, pl.ds(h, 1), :] * st
                                                        + wc[9 + 2 * d, pl.ds(h, 1), :] * tc[h, d, mine, :])
        f_copy(h).start()

    def inside(h):
        cols = pl.ds(pl.multiple_of(h * DK, DK), DK)
        for b in range(2):
            rows = slice(b * BLOCK, (b + 1) * BLOCK)
            cb = col[h, b]
            spread = cb - cb.T
            decay = jnp.where(jj <= ii, jnp.exp(jnp.where(jj <= ii, spread, 0.0)), 0.0)
            qb, kb, vb, gb = q[rows, cols], k[rows, cols], v[rows, cols], g[rows, cols]
            wg = (dot(gb, vb, 1, 1) * decay).astype(BF16)
            wv = (dot(qb, kb, 1, 1) * decay).astype(BF16)
            inner[h, 0, rows, :] = dot(wg, kb, 1, 0)
            inner[h, 1, rows, :] = dot(wg, qb, 0, 0)
            inner[h, 2, rows, :] = dot(wv, gb, 0, 0)

    def outputs(h):
        f_copy(h).wait_recv()
        cols = pl.ds(pl.multiple_of(h * DK, DK), DK)
        e0 = jnp.exp(en[0, pl.ds(h, 1), :])
        e1 = jnp.exp(en[1, pl.ds(h, 1), :])
        sf = fs[h, 0]
        sr = fs[h, 1]
        states = (sf.astype(BF16), (e0 * sf + u0s[h]).astype(BF16))
        grads = ((e1 * sr + v1s[h]).astype(BF16), sr.astype(BF16))
        scale = DK ** -0.5
        for b in range(2):
            rows = slice(b * BLOCK, (b + 1) * BLOCK)
            cb = col[h, b]
            hf = two(jnp.exp(cb))
            tf = two(jnp.exp(cb[BLOCK - 1:BLOCK, :] - cb))
            oq = dot(g[rows, cols], states[b], 1, 1)
            ok = dot(v[rows, cols], grads[b], 1, 1)
            ov = dot(k[rows, cols], grads[b], 1, 0)
            dq[rows, cols] = (scale * (inner[h, 0, rows, :] + hf * oq)).astype(BF16)
            dk[rows, cols] = (scale * (inner[h, 1, rows, :] + tf * ok)).astype(BF16)
            dv[rows, cols] = (scale * (inner[h, 2, rows, :] + tf * ov)).astype(BF16)

    def core_weights():
        c_small().wait_recv()
        me = dc[ic]
        ot = dc[other]
        first = ic == 0
        one = jnp.ones((H, DV), F32)
        zero = jnp.zeros((H, DV), F32)
        eme = jnp.exp(me)
        eot = jnp.exp(ot)
        wc[0] = jnp.where(first, eot, one)
        wc[1] = jnp.where(first, one, eme)
        wc[2] = jnp.where(first, one, eot)
        wc[3] = jnp.where(first, eme, one)
        wc[4] = jnp.where(first, one, eot)
        wc[5] = jnp.where(first, zero, one)
        wc[6] = jnp.where(first, eot, one)
        wc[7] = jnp.where(first, one, zero)
        wc[8] = jnp.where(first, eme, one)
        wc[9] = jnp.where(first, one, zero)
        wc[10] = jnp.where(first, one, eme)
        wc[11] = jnp.where(first, zero, one)
        dx[ix] = me + ot
        for i in (1, 2, 3):
            small(dx, ix, 0, "x", i).start()

    def row_weights():
        for i in (1, 2, 3):
            small(dx, ix, 0, "x", i).wait_recv()
        for j in range(4):
            wx[j] = jnp.exp(dx[j])
        dy[iy] = (dx[0] + dx[1]) + (dx[2] + dx[3])
        for i in (1, 2, 3):
            small(dy, iy, 3, "y", i).start()

    def plane_weights():
        for i in (1, 2, 3):
            small(dy, iy, 3, "y", i).wait_recv()
        for j in range(4):
            wy[j] = jnp.exp(dy[j])
        dz[iz] = (dy[0] + dy[1]) + (dy[2] + dy[3])
        for i in (1, 2, 3):
            small(dz, iz, 6, "z", i).start()

    def prefix_weights():
        for i in (1, 2, 3):
            small(dz, iz, 6, "z", i).wait_recv()
        zero = jnp.zeros((H, DV), F32)
        before = zero
        after = zero
        for j in range(4):
            before = before + jnp.where(j < iy, dy[j], 0.0)
            after = after + jnp.where(j > iy, dy[j], 0.0)
        for j in range(4):
            zf, zr, yf, yr = before, after, zero, zero
            for m in range(4):
                if m > j:
                    zf = zf + jnp.where(m < iz, dz[m], 0.0)
                    yf = yf + jnp.where(m < iy, dy[m], 0.0)
                if m < j:
                    zr = zr + jnp.where(m > iz, dz[m], 0.0)
                    yr = yr + jnp.where(m > iy, dy[m], 0.0)
            wz[j] = jnp.where(j < iz, jnp.exp(zf), 0.0)
            wz[4 + j] = jnp.where(j > iz, jnp.exp(zr), 0.0)
            wz[8 + j] = jnp.where(j < iy, jnp.exp(yf), 0.0)
            wz[12 + j] = jnp.where(j > iy, jnp.exp(yr), 0.0)

    def early_loop(t, carry):
        products(t)
        return carry

    lax.fori_loop(0, EARLY, early_loop, 0)
    pl.semaphore_wait(barrier, 10)
    c_small().start()
    for t in range(EARLY):
        t_copy(t).start()

    def first_loop(t, carry):
        @pl.when(t < H)
        def _():
            products(t)
            t_copy(t).start()

        @pl.when(t == EARLY)
        def _():
            core_weights()

        chip_total(t - EARLY)
        return carry

    lax.fori_loop(EARLY, H + EARLY, first_loop, 0)
    row_weights()

    def second_loop(t, carry):
        @pl.when(t < H)
        def _():
            row_total(t)

        @pl.when(t == 1)
        def _():
            plane_weights()

        @pl.when((t >= 1) & (t < H + 1))
        def _():
            plane_total(t - 1)

        @pl.when(t == 2)
        def _():
            prefix_weights()

        @pl.when(t >= 2)
        def _():
            incoming(t - 2)

        @pl.when(t < H)
        def _():
            inside(t)
        return carry

    lax.fori_loop(0, H + 2, second_loop, 0)

    def third_loop(t, carry):
        @pl.when(t < H)
        def _():
            core_state(t)

        @pl.when(t >= 1)
        def _():
            outputs(t - 1)
        return carry

    lax.fori_loop(0, H + 1, third_loop, 0)

    def drain(h, carry):
        t_copy(h).wait_send()
        f_copy(h).wait_send()
        for i in (1, 2, 3):
            xu_copy(h, i).wait_send()
            y_copy(h, i).wait_send()
            z_copy(h, i).wait_send()
            xd_copy(h, i).wait_send()
        return carry

    lax.fori_loop(0, H, drain, 0)
    c_small().wait_send()
    for i in (1, 2, 3):
        small(dx, ix, 0, "x", i).wait_send()
        small(dy, iy, 3, "y", i).wait_send()
        small(dz, iz, 6, "z", i).wait_send()


def body(queries, keys, values, grad_out, log_decay):
    vmem = pl.BlockSpec(memory_space=pltpu.VMEM)
    hbm = pl.BlockSpec(memory_space=pltpu.HBM)
    shape = pltpu.VMEM(queries.shape, BF16)
    tile = pltpu.VMEM
    dma = pltpu.SemaphoreType.DMA
    return pl.pallas_call(
        kernel,
        out_shape=(shape, shape, shape),
        in_specs=[hbm] * 4 + [vmem],
        out_specs=(vmem, vmem, vmem),
        scratch_shapes=[
            tile(queries.shape, BF16),
            tile(queries.shape, BF16),
            tile(queries.shape, BF16),
            tile(queries.shape, BF16),
            dma((4,)),
            tile((H, 2, BLOCK, BLOCK), F32),
            tile((2, H, DV), F32),
            tile((H, 3, 2 * BLOCK, DK), F32),
            tile((H, DK, DV), F32),
            tile((H, DK, DV), F32),
            tile((H, 2, DK, DV), F32),
            tile((H, 2, DK // 2, DV), F32),
            tile((H, 4, 2, SHARE, DV), F32),
            tile((H, 4, 2, SHARE, DV), F32),
            tile((H, 4, 2, SHARE, DV), F32),
            tile((H, 2, SHARE, DV), F32),
            tile((H, 4, SHARE, DV), F32),
            tile((H, 4, 2, SHARE, DV), F32),
            tile((H, 4, 2, SHARE, DV), F32),
            tile((H, 2, DK // 2, DV), F32),
            tile((H, 2, DK, DV), F32),
            tile((2, H, DV), F32),
            tile((4, H, DV), F32),
            tile((4, H, DV), F32),
            tile((4, H, DV), F32),
            tile((12, H, DV), F32),
            tile((4, H, DV), F32),
            tile((4, H, DV), F32),
            tile((16, H, DV), F32),
            dma((10,)), dma((10,)),
            dma((H,)), dma((H,)),
            dma((H, 3)), dma((H, 3)),
            dma((H, 3)), dma((H, 3)),
            dma((H, 3)), dma((H, 3)),
            dma((H, 3)), dma((H, 3)),
            dma((H,)), dma((H,)),
        ],
        compiler_params=pltpu.CompilerParams(
            collective_id=0, has_side_effects=True, vmem_limit_bytes=50 * 1024 * 1024),
    )(queries, keys, values, grad_out, log_decay)


def solution(mesh):
    torus = Mesh(mesh.devices.reshape(4, 4, 4, 2), AXES)
    rows = P(AXES, None)
    return jax.shard_map(
        body,
        mesh=torus,
        in_specs=(rows, rows, rows, rows, P(None, AXES)),
        out_specs=(rows, rows, rows),
        check_vma=False,
    )
```
